256 devices in a mesh: gx: 8 (over z_lo, core), gy: 32 (over y, x, z_hi).
Axes of the slice: x: 4, y: 4, z: 8 (z_hi: 2, z_lo: 4; z = z_hi * 4 + z_lo), core: 2. Of those that a mesh axis runs over, the one named last changes fastest.
Arguments:
- echoes: bfloat16 [128, 512, 16, 200], P('gx', 'gy'), may hold values from -6 to 6
- start: float32 [200, 32], replicated, may hold values from -6 to 6
- ranks: int32 [8, 32, 1], P('gx', 'gy'), may hold values from 2 to 32
- counts: int32 [8, 32, 1], P('gx', 'gy'), may hold values from 1 to 4
Outputs:
- filtered: bfloat16 [128, 512, 16, 200], P('gx', 'gy')
The draws below stay inside these ranges and needn't reach their ends.
All inputs are finite; a program needn't handle non-finite values.
Results may differ from the reference program's by a relative error of at most 0.0075.
Values may be sent and summed in bfloat16 or wider, within the bound.
No kernel may reach another device: no remote copies, remote signals or barrier semaphores. Data moves between devices by JAX's collectives and lax.ppermute only.
A program may use at most 128 MiB of HBM per device.

```python
import jax
import jax.numpy as jnp
from jax import lax

BS = 16
BZ = 16
NZ = 16
F = 200
K = 32
ITERS = 4
NX = 128
NY = 512
NBZ = 1


def touch_ends(values, own_key, least, largest):
    longest = values.shape.index(max(values.shape))
    spots = []
    for shift in (0, 1):
        where = [jax.random.randint(jax.random.fold_in(own_key, axis), (), 0, length) for axis, length in enumerate(values.shape)]
        where[longest] = (where[longest] + shift) % values.shape[longest]
        spots.append(tuple(where))
    return values.at[spots[0]].set(least).at[spots[1]].set(largest)


def level_of(rng, shape, shards, smallest, high):
    def one(dim, blocks):
        heights = jax.random.uniform(jax.random.fold_in(jax.random.fold_in(rng, 6), dim), (blocks,), jnp.float32, smallest / len(shards), high / len(shards))
        return jnp.repeat(jnp.exp(heights), shape[dim] // blocks).reshape((-1,) + (1,) * (len(shape) - dim - 1))

    factor_of = one(*shards[0])
    for cut in shards[1:]:
        factor_of = factor_of * one(*cut)
    return factor_of


def noise(key, extent, scale, most, pieces=(), kind=jnp.bfloat16):
    array = scale * jax.random.normal(key, extent, jnp.float32)
    if pieces:
        array = array * level_of(key, extent, pieces, -0.22, 0.18)
    return jnp.clip(array, -most, most).astype(kind)


def setup_inputs(seed: int = 0) -> dict:
    key_of = jax.random.split(jax.random.key(seed), 5)
    return {
        "echoes": noise(key_of[0], (NX, NY, NZ, F), 1.0, 6.0, ((0, 8), (1, 32))),
        "start": noise(key_of[1], (F, K), 1.0, 6.0, (), jnp.float32),
        "ranks": touch_ends(jax.random.randint(key_of[2], (NX // BS, NY // BS, NBZ), 2, K + 1), jax.random.fold_in(key_of[2], 1), 2, K).astype(jnp.int32),
        "counts": touch_ends(jax.random.randint(key_of[3], (NX // BS, NY // BS, NBZ), 1, ITERS + 1), jax.random.fold_in(key_of[3], 1), 1, ITERS).astype(jnp.int32),
    }


def tent(offset, span):
    inside = (offset >= 0.0) & (offset < span)
    return jnp.where(inside, 1.0 + jnp.minimum(offset, span - 1.0 - offset), 0.0).astype(jnp.float32)

def segment_grams(region):
    sizex, sizey, depth, frames = region.shape
    half = BZ // 2
    parts = region.reshape(sizex, sizey, depth // half, half, frames).astype(jnp.float32)
    return jnp.einsum('xyshf,xyshg->sfg', parts, parts, precision=lax.Precision.HIGHEST)

def subspace(grams, start, counts):
    basis = jnp.broadcast_to(start, (grams.shape[0],) + start.shape)
    for turn in range(ITERS):
        moved = jnp.einsum('sfg,sgk->sfk', grams, basis, precision=lax.Precision.HIGHEST)
        inner = jnp.einsum('sfk,sfl->skl', moved, moved, precision=lax.Precision.HIGHEST)
        factor = jnp.linalg.cholesky(inner)
        solved = lax.linalg.triangular_solve(factor, moved, left_side=False, lower=True, transpose_a=True)
        basis = jnp.where((turn < counts)[:, None, None], solved, basis)
    return basis

def filter_column(region, segments, ranks, counts, start):
    sizex, sizey, depth, frames = region.shape
    half = BZ // 2
    grams = (segments[:-1] + segments[1:]) / float(sizex * sizey * BZ)
    basis = subspace(grams, start, counts)
    keep = (jnp.arange(K)[None, :] < ranks[:, None]).astype(jnp.float32)
    vectors_all = (basis * keep[:, None, :]).astype(jnp.bfloat16)
    weight = tent(jnp.arange(sizex, dtype=jnp.float32), float(sizex))[:, None, None, None] * tent(jnp.arange(sizey, dtype=jnp.float32), float(sizey))[None, :, None, None] * tent(jnp.arange(BZ, dtype=jnp.float32), float(BZ))[None, None, :, None]

    def add_block(index, total):
        offset = (jnp.asarray(index).astype(jnp.int32) * half).astype(jnp.int32)
        block = lax.dynamic_slice_in_dim(region, offset, BZ, 2)
        vectors = vectors_all[index].astype(jnp.float32)
        coeff = jnp.einsum('xyzf,fk->xyzk', block.astype(jnp.float32), vectors, precision=lax.Precision.HIGHEST).astype(jnp.bfloat16)
        clutter = jnp.einsum('xyzk,fk->xyzf', coeff.astype(jnp.float32), vectors, precision=lax.Precision.HIGHEST)
        contrib = weight * (block.astype(jnp.float32) - clutter)
        previous = lax.dynamic_slice_in_dim(total, offset, BZ, 2)
        return lax.dynamic_update_slice_in_dim(total, previous + contrib, offset, 2)
    return lax.fori_loop(0, grams.shape[0], add_block, jnp.zeros(region.shape, jnp.float32))

def reference(echoes, start, ranks, counts):
    sizex, sizey, depth, frames = echoes.shape
    grid_x = sizex // BS
    grid_y = sizey // BS
    columns = grid_y - 1
    zero = jnp.zeros((), jnp.int32)

    def visit(index, total):
        index = jnp.asarray(index).astype(jnp.int32)
        blockx = index // columns
        blocky = index % columns
        anchor = (blockx * BS, blocky * BS, zero, zero)
        region = lax.dynamic_slice(echoes, anchor, (2 * BS, 2 * BS, depth, frames))
        part = filter_column(region, segment_grams(region), ranks[blockx, blocky], counts[blockx, blocky], start)
        previous = lax.dynamic_slice(total, anchor, part.shape)
        return lax.dynamic_update_slice(total, previous + part, anchor)
    total = lax.fori_loop(0, (grid_x - 1) * columns, visit, jnp.zeros(echoes.shape, jnp.float32))
    span = float(2 * BS)
    posx = jnp.arange(sizex, dtype=jnp.float32)
    posy = jnp.arange(sizey, dtype=jnp.float32)
    posz = jnp.arange(depth, dtype=jnp.float32)
    coverx = jnp.sum(tent(posx[None, :] - BS * jnp.arange(grid_x - 1, dtype=jnp.float32)[:, None], span), axis=0)
    covery = jnp.sum(tent(posy[None, :] - BS * jnp.arange(grid_y - 1, dtype=jnp.float32)[:, None], span), axis=0)
    nblocks = 2 * depth // BZ - 1
    coverz = jnp.sum(tent(posz[None, :] - BZ // 2 * jnp.arange(nblocks, dtype=jnp.float32)[:, None], float(BZ)), axis=0)
    cover = coverx[:, None, None, None] * covery[None, :, None, None] * coverz[None, None, :, None]
    return (total / cover).astype(jnp.bfloat16)
```

```python
import functools

import jax
import jax.numpy as jnp
from jax import lax
from jax.experimental import pallas as pl
from jax.experimental.pallas import tpu as pltpu
from jax.sharding import PartitionSpec as P

BZ = 16
K = 32
ITERS = 4
LANES = 128
META = 8
GRAM_CHUNK = 1024
PROJ_CHUNK = 512
PANEL = 16

f32 = jnp.float32
bf16 = jnp.bfloat16


def iota(shape, dim):
    return lax.broadcasted_iota(jnp.int32, shape, dim)


def gram_kernel(rank_ref, count_ref, c_ref, own_ref, sent_ref, acc_ref):
    step = pl.program_id(0)
    frames = acc_ref.shape[0]
    c = c_ref[...]
    part = lax.dot_general(c, c, (((0,), (0,)), ((), ())), preferred_element_type=f32)

    @pl.when(step == 0)
    def _():
        acc_ref[...] = part

    @pl.when(step > 0)
    def _():
        acc_ref[...] += part

    @pl.when(step == pl.num_programs(0) - 1)
    def _():
        rest = frames - LANES
        first = LANES - rest
        own_ref[...] = acc_ref[:, :LANES]
        shape = (rest, rest)
        low = iota(shape, 1) <= iota(shape, 0)
        own_ref[first:LANES, :rest] = jnp.where(
            low, acc_ref[LANES:, LANES:], acc_ref[first:LANES, :rest]
        )
        tile = own_ref[META : META + 8, :]
        row, lane = iota(tile.shape, 0), iota(tile.shape, 1)
        rank = rank_ref[0].astype(f32)
        count = count_ref[0].astype(f32)
        tile = jnp.where((row == 0) & (lane == 0), rank, tile)
        tile = jnp.where((row == 0) & (lane == 1), count, tile)
        own_ref[META : META + 8, :] = tile
        sent_ref[...] = own_ref[...].astype(bf16)


def own_gram(voxels, rank, count):
    m, frames = voxels.shape
    steps = m // GRAM_CHUNK
    return pl.pallas_call(
        gram_kernel,
        grid=(steps,),
        in_specs=[
            pl.BlockSpec(memory_space=pltpu.SMEM),
            pl.BlockSpec(memory_space=pltpu.SMEM),
            pl.BlockSpec((GRAM_CHUNK, frames), lambda i: (i, 0)),
        ],
        out_specs=[
            pl.BlockSpec((frames, LANES), lambda i: (0, 0)),
            pl.BlockSpec((frames, LANES), lambda i: (0, 0)),
        ],
        out_shape=[
            jax.ShapeDtypeStruct((frames, LANES), f32),
            jax.ShapeDtypeStruct((frames, LANES), bf16),
        ],
        scratch_shapes=[pltpu.VMEM((frames, frames), f32)],
        compiler_params=pltpu.CompilerParams(dimension_semantics=("arbitrary",)),
        cost_estimate=pl.CostEstimate(
            flops=2 * m * frames * frames, bytes_accessed=2 * m * frames, transcendentals=0
        ),
        name="own_gram",
    )(rank, count, voxels)


def split(x):
    high = x.astype(bf16)
    low = (x - high.astype(f32)).astype(bf16)
    return high, low


def unpacked(pk):
    frames = pk.shape[0]
    rest = frames - LANES
    first = LANES - rest
    shape = (LANES, LANES)
    row, lane = iota(shape, 0), iota(shape, 1)
    gap = jnp.zeros((first, LANES), f32)
    top = pk[:LANES]
    g11 = jnp.where(lane >= row, top, top.T)
    g21 = jnp.concatenate([pk[LANES:], gap], 0)
    low = jnp.concatenate([pk[first:LANES], gap], 0)
    low = jnp.where((lane <= row) & (row < rest), low, 0.0)
    g22 = jnp.where(lane <= row, low, low.T)
    return g11, g21.T, g21, g22


def spread(x, row):
    return jnp.broadcast_to(x[row : row + 1, :], (8, LANES))


def inverse_factor(a):
    count = K // 8
    sub, lane = iota((8, LANES), 0), iota((8, LANES), 1)
    base = (lane // K) * K
    rows = [a[8 * v : 8 * v + 8] for v in range(count)]
    inv = [jnp.where(sub + 8 * v == lane - base, 1.0, 0.0) for v in range(count)]
    for k0 in range(0, K, PANEL):
        cols = {
            k: {
                v: jnp.take_along_axis(rows[v], base + k, axis=1)
                for v in range(k0 // 8, count)
            }
            for k in range(k0, k0 + PANEL)
        }
        for j in range(k0, k0 + PANEL):
            vj, sj = j // 8, j % 8
            r = lax.rsqrt(spread(cols[j][vj], sj))
            fac = {v: cols[j][v] * r for v in range(vj, count)}
            fac[vj] = jnp.where(sub > sj, fac[vj], 0.0)
            for k in range(j + 1, k0 + PANEL):
                m = spread(fac[k // 8], k % 8)
                for v in range(k // 8, count):
                    cols[k][v] = cols[k][v] - fac[v] * m
            e = spread(inv[vj], sj) * r
            for v in range(vj, count):
                inv[v] = inv[v] - fac[v] * e
            inv[vj] = jnp.where(sub == sj, e, inv[vj])
            if k0 + PANEL < K:
                e = spread(rows[vj], sj) * r
                for v in range(vj, count):
                    rows[v] = rows[v] - fac[v] * e
    return jnp.concatenate(inv, 0)


def blockwise(parts_of):
    return jnp.concatenate([parts_of(b) for b in range(4)], 0)


def scalar_at(tile, lane_at):
    row, lane = iota(tile.shape, 0), iota(tile.shape, 1)
    return jnp.sum(jnp.where((row == 0) & (lane == lane_at), tile, 0.0)).astype(jnp.int32)


def subspaces(rows, cols, sums_ref, near_ref, far_ref, start_ref, high_ref, low_ref, z_ref, v_ref):
    row, col = lax.axis_index("gx"), lax.axis_index("gy")
    scale = 1.0 / float(BZ * BZ * BZ * 4)
    group = iota((K, LANES), 1) // K
    ranks, counts = [], []
    s_high, s_low = split(start_ref[...])
    s_both = jnp.concatenate([s_high, s_low], 0)
    for b in range(4):
        slot, turn_x = b % 2, b // 2
        other_ref = near_ref if turn_x == 0 else far_ref
        other = other_ref[slot]
        pk = (sums_ref[slot] + other.astype(f32)) * scale
        g11, g12, g21, g22 = unpacked(pk)
        for ref, part in ((high_ref, 0), (low_ref, 1)):
            ref[b, :LANES, :LANES] = split(g11)[part]
            ref[b, :LANES, LANES:] = split(g12)[part]
            ref[b, LANES:, :LANES] = split(g21)[part]
            ref[b, LANES:, LANES:] = split(g22)[part]
        right = lax.rem(col, 2) == slot
        down = lax.rem(row, 2) == turn_x
        tile = jnp.where(
            down,
            sums_ref[slot, META : META + 8, :],
            other_ref[slot, 0:16, :].astype(f32)[META : META + 8],
        )
        last_y = jnp.where(right, cols - 1, 0)
        last_x = jnp.where(down, rows - 1, 0)
        rank = jnp.where(col == last_y, 0, scalar_at(tile, 0))
        ranks.append(jnp.where(row == last_x, 0, rank))
        counts.append(scalar_at(tile, 1))
    for b in range(4):
        both = jnp.dot(s_both, high_ref[b], preferred_element_type=f32)
        z_ref[K * b : K * b + K, :] = (
            both[:K] + both[K:] + jnp.dot(s_high, low_ref[b], preferred_element_type=f32)
        )

    def turn(t, carry):
        z_high, z_low = split(z_ref[...])
        zz = jnp.concatenate([z_high, z_low], 0)
        s = lax.dot_general(zz, zz, (((1,), (1,)), ((), ())), preferred_element_type=f32)
        half = 4 * K
        s = (s[:half, :half] + s[half:, half:]) + (s[:half, half:] + s[half:, :half])
        a = jnp.where(group == 0, s[:K], 0.0)
        for b in range(1, 4):
            a = jnp.where(group == b, s[K * b : K * b + K], a)
        moved = []
        for b in range(4):
            high = z_high[K * b : K * b + K]
            low = z_low[K * b : K * b + K]
            both = jnp.dot(
                jnp.concatenate([high, low], 0), high_ref[b], preferred_element_type=f32
            )
            moved.append(
                both[:K] + both[K:] + jnp.dot(high, low_ref[b], preferred_element_type=f32)
            )
        y_high, y_low = split(jnp.concatenate(moved, 0))
        yy = jnp.concatenate([y_high, y_low], 0)
        inv = inverse_factor(a)
        wide = blockwise(lambda b: jnp.where(group == b, inv, 0.0))
        i_high, i_low = split(wide)
        left = jnp.concatenate(
            [jnp.concatenate([i_high, i_high], 1), jnp.concatenate([i_low, i_low], 1)], 0
        )
        nxt = jnp.dot(left, yy, preferred_element_type=f32)
        z_ref[...] = nxt[:half] + nxt[half:]
        v = jnp.dot(left, zz, preferred_element_type=f32)
        v = v[:half] + v[half:]
        for b in range(4):
            part = slice(K * b, K * b + K)

            @pl.when(counts[b] == t + 1)
            def _():
                v_ref[part, :] = v[part]

        return carry

    lax.fori_loop(0, ITERS, turn, 0)
    k = iota((K, v_ref.shape[1]), 0)
    return blockwise(lambda b: jnp.where(k < ranks[b], v_ref[K * b : K * b + K, :], 0.0)).astype(bf16)


def tents(rows, cols, span):
    row, col = lax.axis_index("gx"), lax.axis_index("gy")

    def share(far, position, at, last):
        first_edge = jnp.where(at == 0, 1.0, 0.0)
        last_edge = jnp.where(at == last, 1.0, 0.0)
        edge = jnp.maximum(first_edge, last_edge)
        tent = jnp.where(far, float(span) - position, position + 1.0) / float(span + 1)
        tent = tent * (1.0 - edge) + edge
        return tent * jnp.where(far, 1.0 - first_edge, 1.0 - last_edge)

    def along_x(offset):
        far = iota((8, LANES), 1) // (2 * K) != lax.rem(row, 2)
        return share(far, offset.astype(f32), row, rows - 1)

    group = iota((span, LANES), 1) // K
    far = group % 2 != lax.rem(col, 2)
    along_y = share(far, iota((span, LANES), 0).astype(f32), col, cols - 1)
    return along_x, along_y


def filter_kernel(
    rows, cols, span, sums_ref, near_ref, far_ref, start_ref, c_ref, out_ref, high_ref, low_ref, z_ref, v_ref, q_ref
):
    step = pl.program_id(0)
    frames = c_ref.shape[1]

    @pl.when(step == 0)
    def _():
        q_ref[...] = subspaces(
            rows, cols, sums_ref, near_ref, far_ref, start_ref, high_ref, low_ref, z_ref, v_ref
        )

    along_x, along_y = tents(rows, cols, span)
    q = q_ref[:, :frames]
    area = span * BZ
    per_step = c_ref.shape[0] // area
    for i in range(per_step):
        c = c_ref[i * area : (i + 1) * area, :]
        p = lax.dot_general(c, q, (((1,), (1,)), ((), ())), preferred_element_type=f32)
        wx = along_x(step * per_step + i)[:1]
        weight = along_y * wx
        p = p.reshape(span, BZ, LANES) * weight[:, None, :]
        p = p.reshape(area, LANES).astype(bf16)
        clutter = jnp.dot(p, q, preferred_element_type=f32)
        out_ref[i * area : (i + 1) * area, :] = (c.astype(f32) - clutter).astype(bf16)


def filtered(voxels, sums, near, far, start, rows, cols, span):
    m, frames = voxels.shape
    whole3 = pl.BlockSpec(sums.shape, lambda i: (0, 0, 0))
    chunk = pl.BlockSpec((PROJ_CHUNK, frames), lambda i: (i, 0))
    return pl.pallas_call(
        functools.partial(filter_kernel, rows, cols, span),
        grid=(m // PROJ_CHUNK,),
        in_specs=[whole3, whole3, whole3, pl.BlockSpec(start.shape, lambda i: (0, 0)), chunk],
        out_specs=chunk,
        out_shape=jax.ShapeDtypeStruct((m, frames), bf16),
        scratch_shapes=[
            pltpu.VMEM((4, 2 * LANES, 2 * LANES), bf16),
            pltpu.VMEM((4, 2 * LANES, 2 * LANES), bf16),
            pltpu.VMEM((4 * K, 2 * LANES), f32),
            pltpu.VMEM((4 * K, 2 * LANES), f32),
            pltpu.VMEM((4 * K, 2 * LANES), bf16),
        ],
        compiler_params=pltpu.CompilerParams(dimension_semantics=("arbitrary",)),
        cost_estimate=pl.CostEstimate(
            flops=8 * m * frames * K * 4, bytes_accessed=4 * m * frames, transcendentals=0
        ),
        name="filtered",
    )(sums, near, far, start, voxels)


def partner(x, axis):
    n = lax.axis_size(axis)
    return lax.ppermute(x, axis, [(i, i ^ 1) for i in range(n)])


def outer_partner(x, axis):
    n = lax.axis_size(axis)
    return lax.ppermute(x, axis, [(i, ((i - 1) ^ 1) + 1) for i in range(1, n - 1)])


def handed_on(x):
    n = lax.axis_size("gy")
    route = [(i, i + 2) for i in range(0, n - 2, 2)] + [(i, i - 2) for i in range(3, n, 2)]
    return lax.ppermute(x, "gy", route)


def body(echoes, start, ranks, counts):
    span, _, depth, frames = echoes.shape
    rows, cols = lax.axis_size("gx"), lax.axis_size("gy")
    voxels = echoes.reshape(span * span * depth, frames)
    own, sent = own_gram(voxels, ranks.reshape(1), counts.reshape(1))
    near = partner(sent, "gy")
    far = handed_on(near)
    even = lax.rem(lax.axis_index("gy"), 2) == 0
    near32, far32 = near.astype(f32), far.astype(f32)
    pair = jnp.stack([own + near32, own + far32])
    meta = jnp.stack([jnp.where(even, own, near32), jnp.where(even, far32, own)])
    at = (iota(pair.shape, 1) == META) & (iota(pair.shape, 2) < 2)
    pair = jnp.where(at, meta, pair)
    sent = pair.astype(bf16)
    near = partner(sent, "gx")
    far = outer_partner(sent, "gx")
    basis = jnp.pad(start.T, ((0, 0), (0, 2 * LANES - frames)))
    out = filtered(voxels, pair, near, far, basis, rows, cols, span)
    return out.reshape(echoes.shape)


def solution(mesh):
    placed = (P("gx", "gy", None, None), P(), P("gx", "gy", None), P("gx", "gy", None))
    return jax.shard_map(
        body, mesh=mesh, in_specs=placed, out_specs=P("gx", "gy", None, None), check_vma=False
    )
```

```python
import functools

import jax
import jax.numpy as jnp
from jax import lax
from jax.experimental import pallas as pl
from jax.experimental.pallas import tpu as pltpu
from jax.sharding import PartitionSpec as P

BZ = 16
K = 32
ITERS = 4
LANES = 128
META = 8
GRAM_CHUNK = 1024
PROJ_CHUNK = 512
VMEM_LIMIT = 56_000_000
PANEL = 16

f32 = jnp.float32
bf16 = jnp.bfloat16


def iota(shape, dim):
    return lax.broadcasted_iota(jnp.int32, shape, dim)


def gram_kernel(
    rank_hbm, count_hbm, c_hbm, own_ref, sent_ref, rank_ref, count_ref, c_ref, acc_ref, sems, few_sems
):
    m, frames = c_ref.shape
    few = [
        pltpu.make_async_copy(rank_hbm, rank_ref, few_sems.at[0]),
        pltpu.make_async_copy(count_hbm, count_ref, few_sems.at[1]),
    ]
    loads = []
    for i in range(m // GRAM_CHUNK):
        part = pl.ds(i * GRAM_CHUNK, GRAM_CHUNK)
        loads.append(pltpu.make_async_copy(c_hbm.at[part], c_ref.at[part], sems.at[i]))
        loads[-1].start()
    for load in few:
        load.start()
    for i, load in enumerate(loads):
        load.wait()
        c = c_ref[i * GRAM_CHUNK : (i + 1) * GRAM_CHUNK, :]
        part = lax.dot_general(c, c, (((0,), (0,)), ((), ())), preferred_element_type=f32)
        if i == 0:
            acc_ref[...] = part
        else:
            acc_ref[...] += part
    for load in few:
        load.wait()
    rest = frames - LANES
    first = LANES - rest
    own_ref[...] = acc_ref[:, :LANES]
    shape = (rest, rest)
    low = iota(shape, 1) <= iota(shape, 0)
    own_ref[first:LANES, :rest] = jnp.where(
        low, acc_ref[LANES:, LANES:], acc_ref[first:LANES, :rest]
    )
    tile = own_ref[META : META + 8, :]
    row, lane = iota(tile.shape, 0), iota(tile.shape, 1)
    rank = jnp.broadcast_to(rank_ref[0].astype(f32), tile.shape)
    count = jnp.broadcast_to(count_ref[0].astype(f32), tile.shape)
    tile = jnp.where((row == 0) & (lane == 0), rank, tile)
    tile = jnp.where((row == 0) & (lane == 1), count, tile)
    own_ref[META : META + 8, :] = tile
    sent_ref[...] = own_ref[...].astype(bf16)


def vmem():
    return pl.BlockSpec(memory_space=pltpu.VMEM)


def hbm():
    return pl.BlockSpec(memory_space=pltpu.HBM)


def own_gram(voxels, rank, count):
    m, frames = voxels.shape
    return pl.pallas_call(
        gram_kernel,
        in_specs=[hbm()] * 3,
        out_specs=[vmem(), vmem()],
        out_shape=[
            jax.ShapeDtypeStruct((frames, LANES), f32),
            jax.ShapeDtypeStruct((frames, LANES), bf16),
        ],
        scratch_shapes=[
            pltpu.VMEM(rank.shape, jnp.int32),
            pltpu.VMEM(count.shape, jnp.int32),
            pltpu.VMEM((m, frames), bf16),
            pltpu.VMEM((frames, frames), f32),
            pltpu.SemaphoreType.DMA((m // GRAM_CHUNK,)),
            pltpu.SemaphoreType.DMA((2,)),
        ],
        compiler_params=pltpu.CompilerParams(vmem_limit_bytes=VMEM_LIMIT),
        cost_estimate=pl.CostEstimate(
            flops=2 * m * frames * frames, bytes_accessed=2 * m * frames, transcendentals=0
        ),
        name="own_gram",
    )(rank, count, voxels)


def pair_kernel(own_ref, near_ref, far_ref, pair_ref, sent_ref):
    even = lax.rem(lax.axis_index("gy"), 2) == 0
    own = own_ref[...]
    at = slice(META, META + 8)
    shape = (8, own.shape[1])
    spot = (iota(shape, 0) == 0) & (iota(shape, 1) < 2)
    for slot, other_ref in ((0, near_ref), (1, far_ref)):
        other = other_ref[...].astype(f32)
        total = own + other
        pair_ref[slot] = total
        right = even if slot == 0 else jnp.logical_not(even)
        meta = jnp.where(right, own[at], other[at])
        pair_ref[slot, at, :] = jnp.where(spot, meta, total[at])
        sent_ref[slot] = pair_ref[slot].astype(bf16)


def pair_sums(own, near, far):
    shape = (2,) + own.shape
    return pl.pallas_call(
        pair_kernel,
        in_specs=[vmem()] * 3,
        out_specs=[vmem()] * 2,
        out_shape=[jax.ShapeDtypeStruct(shape, f32), jax.ShapeDtypeStruct(shape, bf16)],
        compiler_params=pltpu.CompilerParams(vmem_limit_bytes=VMEM_LIMIT),
        cost_estimate=pl.CostEstimate(flops=4 * own.size, bytes_accessed=0, transcendentals=0),
        name="pair_sums",
    )(own, near, far)


def split(x):
    high = x.astype(bf16)
    low = (x - high.astype(f32)).astype(bf16)
    return high, low


def unpacked(pk):
    frames = pk.shape[0]
    rest = frames - LANES
    first = LANES - rest
    shape = (LANES, LANES)
    row, lane = iota(shape, 0), iota(shape, 1)
    gap = jnp.zeros((first, LANES), f32)
    top = pk[:LANES]
    g11 = jnp.where(lane >= row, top, top.T)
    g21 = jnp.concatenate([pk[LANES:], gap], 0)
    low = jnp.concatenate([pk[first:LANES], gap], 0)
    low = jnp.where((lane <= row) & (row < rest), low, 0.0)
    g22 = jnp.where(lane <= row, low, low.T)
    return g11, g21.T, g21, g22


def spread(x, row):
    return jnp.broadcast_to(x[row : row + 1, :], (8, LANES))


def inverse_factor(a):
    count = K // 8
    sub, lane = iota((8, LANES), 0), iota((8, LANES), 1)
    base = (lane // K) * K
    rows = [a[8 * v : 8 * v + 8] for v in range(count)]
    inv = [jnp.where(sub + 8 * v == lane - base, 1.0, 0.0) for v in range(count)]
    for k0 in range(0, K, PANEL):
        cols = {
            k: {
                v: jnp.take_along_axis(rows[v], base + k, axis=1)
                for v in range(k0 // 8, count)
            }
            for k in range(k0, k0 + PANEL)
        }
        for j in range(k0, k0 + PANEL):
            vj, sj = j // 8, j % 8
            r = lax.rsqrt(spread(cols[j][vj], sj))
            fac = {v: cols[j][v] * r for v in range(vj, count)}
            fac[vj] = jnp.where(sub > sj, fac[vj], 0.0)
            for k in range(j + 1, k0 + PANEL):
                m = spread(fac[k // 8], k % 8)
                for v in range(k // 8, count):
                    cols[k][v] = cols[k][v] - fac[v] * m
            e = spread(inv[vj], sj) * r
            for v in range(vj, count):
                inv[v] = inv[v] - fac[v] * e
            inv[vj] = jnp.where(sub == sj, e, inv[vj])
            if k0 + PANEL < K:
                e = spread(rows[vj], sj) * r
                for v in range(vj, count):
                    rows[v] = rows[v] - fac[v] * e
    return jnp.concatenate(inv, 0)


def blockwise(parts_of):
    return jnp.concatenate([parts_of(b) for b in range(4)], 0)


def scalar_at(tile, lane_at):
    row, lane = iota(tile.shape, 0), iota(tile.shape, 1)
    return jnp.sum(jnp.where((row == 0) & (lane == lane_at), tile, 0.0)).astype(jnp.int32)


def subspaces(rows, cols, sums_ref, near_ref, far_ref, start_ref, high_ref, low_ref, z_ref, v_ref):
    row, col = lax.axis_index("gx"), lax.axis_index("gy")
    scale = 1.0 / float(BZ * BZ * BZ * 4)
    group = iota((K, LANES), 1) // K
    ranks, counts = [], []
    s_high, s_low = split(start_ref[...])
    s_both = jnp.concatenate([s_high, s_low], 0)
    for b in range(4):
        slot, turn_x = b % 2, b // 2
        other_ref = near_ref if turn_x == 0 else far_ref
        other = other_ref[slot]
        pk = (sums_ref[slot] + other.astype(f32)) * scale
        g11, g12, g21, g22 = unpacked(pk)
        for ref, part in ((high_ref, 0), (low_ref, 1)):
            ref[b, :LANES, :LANES] = split(g11)[part]
            ref[b, :LANES, LANES:] = split(g12)[part]
            ref[b, LANES:, :LANES] = split(g21)[part]
            ref[b, LANES:, LANES:] = split(g22)[part]
        right = lax.rem(col, 2) == slot
        down = lax.rem(row, 2) == turn_x
        tile = jnp.where(
            down,
            sums_ref[slot, META : META + 8, :],
            other_ref[slot, 0:16, :].astype(f32)[META : META + 8],
        )
        last_y = jnp.where(right, cols - 1, 0)
        last_x = jnp.where(down, rows - 1, 0)
        rank = jnp.where(col == last_y, 0, scalar_at(tile, 0))
        ranks.append(jnp.where(row == last_x, 0, rank))
        counts.append(scalar_at(tile, 1))
    for b in range(4):
        both = jnp.dot(s_both, high_ref[b], preferred_element_type=f32)
        z_ref[K * b : K * b + K, :] = (
            both[:K] + both[K:] + jnp.dot(s_high, low_ref[b], preferred_element_type=f32)
        )

    def turn(t, carry):
        z_high, z_low = split(z_ref[...])
        zz = jnp.concatenate([z_high, z_low], 0)
        s = lax.dot_general(zz, zz, (((1,), (1,)), ((), ())), preferred_element_type=f32)
        half = 4 * K
        s = (s[:half, :half] + s[half:, half:]) + (s[:half, half:] + s[half:, :half])
        a = jnp.where(group == 0, s[:K], 0.0)
        for b in range(1, 4):
            a = jnp.where(group == b, s[K * b : K * b + K], a)
        moved = []
        for b in range(4):
            high = z_high[K * b : K * b + K]
            low = z_low[K * b : K * b + K]
            both = jnp.dot(
                jnp.concatenate([high, low], 0), high_ref[b], preferred_element_type=f32
            )
            moved.append(
                both[:K] + both[K:] + jnp.dot(high, low_ref[b], preferred_element_type=f32)
            )
        y_high, y_low = split(jnp.concatenate(moved, 0))
        yy = jnp.concatenate([y_high, y_low], 0)
        inv = inverse_factor(a)
        wide = blockwise(lambda b: jnp.where(group == b, inv, 0.0))
        i_high, i_low = split(wide)
        left = jnp.concatenate(
            [jnp.concatenate([i_high, i_high], 1), jnp.concatenate([i_low, i_low], 1)], 0
        )
        nxt = jnp.dot(left, yy, preferred_element_type=f32)
        z_ref[...] = nxt[:half] + nxt[half:]
        v = jnp.dot(left, zz, preferred_element_type=f32)
        v = v[:half] + v[half:]
        for b in range(4):
            part = slice(K * b, K * b + K)

            @pl.when(counts[b] == t + 1)
            def _():
                v_ref[part, :] = v[part]

        return carry

    lax.fori_loop(0, ITERS, turn, 0)
    k = iota((K, v_ref.shape[1]), 0)
    return blockwise(lambda b: jnp.where(k < ranks[b], v_ref[K * b : K * b + K, :], 0.0)).astype(bf16)


def tents(rows, cols, span):
    row, col = lax.axis_index("gx"), lax.axis_index("gy")

    def share(far, position, at, last):
        first_edge = jnp.where(at == 0, 1.0, 0.0)
        last_edge = jnp.where(at == last, 1.0, 0.0)
        edge = jnp.maximum(first_edge, last_edge)
        tent = jnp.where(far, float(span) - position, position + 1.0) / float(span + 1)
        tent = tent * (1.0 - edge) + edge
        return tent * jnp.where(far, 1.0 - first_edge, 1.0 - last_edge)

    def along_x(offset):
        far = iota((8, LANES), 1) // (2 * K) != lax.rem(row, 2)
        return share(far, offset, row, rows - 1)

    group = iota((span, LANES), 1) // K
    far = group % 2 != lax.rem(col, 2)
    along_y = share(far, iota((span, LANES), 0).astype(f32), col, cols - 1)
    return along_x, along_y


def filter_kernel(
    rows,
    cols,
    span,
    sums_ref,
    near_ref,
    far_ref,
    start_ref,
    c_hbm,
    out_hbm,
    high_ref,
    low_ref,
    z_ref,
    v_ref,
    c_ref,
    out_ref,
    in_sems,
    out_sems,
):
    m, frames = c_ref.shape
    chunks = [pl.ds(i * PROJ_CHUNK, PROJ_CHUNK) for i in range(m // PROJ_CHUNK)]
    loads = [
        pltpu.make_async_copy(c_hbm.at[part], c_ref.at[part], in_sems.at[i])
        for i, part in enumerate(chunks)
    ]
    stores = [
        pltpu.make_async_copy(out_ref.at[part], out_hbm.at[part], out_sems.at[i])
        for i, part in enumerate(chunks)
    ]
    for load in loads:
        load.start()
    q = subspaces(rows, cols, sums_ref, near_ref, far_ref, start_ref, high_ref, low_ref, z_ref, v_ref)
    q = q[:, :frames]
    along_x, along_y = tents(rows, cols, span)
    area = span * BZ
    for load in loads:
        load.wait()
    for at in range(0, m, area):
        c = c_ref[at : at + area, :]
        p = lax.dot_general(c, q, (((1,), (1,)), ((), ())), preferred_element_type=f32)
        weight = along_y * along_x(float(at // area))[:1]
        p = p.reshape(span, BZ, LANES) * weight[:, None, :]
        p = p.reshape(area, LANES).astype(bf16)
        clutter = jnp.dot(p, q, preferred_element_type=f32)
        out_ref[at : at + area, :] = (c.astype(f32) - clutter).astype(bf16)
        if (at + area) % PROJ_CHUNK == 0:
            stores[at // PROJ_CHUNK].start()
    for store in stores:
        store.wait()


def filtered(voxels, sums, near, far, start, rows, cols, span):
    m, frames = voxels.shape
    return pl.pallas_call(
        functools.partial(filter_kernel, rows, cols, span),
        in_specs=[vmem()] * 4 + [hbm()],
        out_specs=hbm(),
        out_shape=jax.ShapeDtypeStruct((m, frames), bf16),
        scratch_shapes=[
            pltpu.VMEM((4, 2 * LANES, 2 * LANES), bf16),
            pltpu.VMEM((4, 2 * LANES, 2 * LANES), bf16),
            pltpu.VMEM((4 * K, 2 * LANES), f32),
            pltpu.VMEM((4 * K, 2 * LANES), f32),
            pltpu.VMEM((m, frames), bf16),
            pltpu.VMEM((m, frames), bf16),
            pltpu.SemaphoreType.DMA((m // PROJ_CHUNK,)),
            pltpu.SemaphoreType.DMA((m // PROJ_CHUNK,)),
        ],
        compiler_params=pltpu.CompilerParams(vmem_limit_bytes=VMEM_LIMIT),
        cost_estimate=pl.CostEstimate(
            flops=8 * m * frames * K * 4, bytes_accessed=4 * m * frames, transcendentals=0
        ),
        name="filtered",
    )(sums, near, far, start, voxels)


def partner(x, axis):
    n = lax.axis_size(axis)
    return lax.ppermute(x, axis, [(i, i ^ 1) for i in range(n)])


def outer_partner(x, axis):
    n = lax.axis_size(axis)
    return lax.ppermute(x, axis, [(i, ((i - 1) ^ 1) + 1) for i in range(1, n - 1)])


def handed_on(x):
    n = lax.axis_size("gy")
    route = [(i, i + 2) for i in range(0, n - 2, 2)] + [(i, i - 2) for i in range(3, n, 2)]
    return lax.ppermute(x, "gy", route)


def body(echoes, start, ranks, counts):
    span, _, depth, frames = echoes.shape
    rows, cols = lax.axis_size("gx"), lax.axis_size("gy")
    voxels = echoes.reshape(span * span * depth, frames)
    own, sent = own_gram(voxels, ranks, counts)
    near = partner(sent, "gy")
    far = handed_on(near)
    pair, sent = pair_sums(own, near, far)
    near = partner(sent, "gx")
    far = outer_partner(sent, "gx")
    basis = jnp.pad(start.T, ((0, 0), (0, 2 * LANES - frames)))
    out = filtered(voxels, pair, near, far, basis, rows, cols, span)
    return out.reshape(echoes.shape)


def solution(mesh):
    placed = (P("gx", "gy", None, None), P(), P("gx", "gy", None), P("gx", "gy", None))
    return jax.shard_map(
        body, mesh=mesh, in_specs=placed, out_specs=P("gx", "gy", None, None), check_vma=False
    )
```

```python
import functools

import jax
import jax.numpy as jnp
from jax import lax
from jax.experimental import pallas as pl
from jax.experimental.pallas import tpu as pltpu
from jax.sharding import PartitionSpec as P

BZ = 16
K = 32
ITERS = 4
LANES = 128
META = 8
LOAD_ROWS = 512
GRAM_ROWS = (2560, 1536)
PROJ_CHUNK = 512
VMEM_LIMIT = 55_500_000
PANEL = 16

f32 = jnp.float32
bf16 = jnp.bfloat16


def iota(shape, dim):
    return lax.broadcasted_iota(jnp.int32, shape, dim)


def gram_kernel(c_hbm, own_ref, c_ref, acc_ref, sems):
    m, frames = c_ref.shape
    loads = []
    for i in range(m // LOAD_ROWS):
        part = pl.ds(i * LOAD_ROWS, LOAD_ROWS)
        loads.append(pltpu.make_async_copy(c_hbm.at[part], c_ref.at[part], sems.at[i]))
        loads[-1].start()
    first = 0
    for i, size in enumerate(GRAM_ROWS):
        for load in loads[first // LOAD_ROWS : (first + size) // LOAD_ROWS]:
            load.wait()
        c = c_ref[first : first + size, :]
        part = lax.dot_general(c, c, (((0,), (0,)), ((), ())), preferred_element_type=f32)
        if i == 0:
            acc_ref[...] = part
        else:
            acc_ref[...] += part
        first += size
    rest = frames - LANES
    first = LANES - rest
    own_ref[...] = acc_ref[:, :LANES]
    shape = (rest, rest)
    low = iota(shape, 1) <= iota(shape, 0)
    own_ref[first:LANES, :rest] = jnp.where(
        low, acc_ref[LANES:, LANES:], acc_ref[first:LANES, :rest]
    )


def vmem():
    return pl.BlockSpec(memory_space=pltpu.VMEM)


def hbm():
    return pl.BlockSpec(memory_space=pltpu.HBM)


def own_gram(voxels):
    m, frames = voxels.shape
    return pl.pallas_call(
        gram_kernel,
        in_specs=[hbm()],
        out_specs=vmem(),
        out_shape=jax.ShapeDtypeStruct((frames, LANES), f32),
        scratch_shapes=[
            pltpu.VMEM((m, frames), bf16),
            pltpu.VMEM((frames, frames), f32),
            pltpu.SemaphoreType.DMA((m // LOAD_ROWS,)),
        ],
        compiler_params=pltpu.CompilerParams(vmem_limit_bytes=VMEM_LIMIT),
        cost_estimate=pl.CostEstimate(
            flops=2 * m * frames * frames, bytes_accessed=2 * m * frames, transcendentals=0
        ),
        name="own_gram",
    )(voxels)


def pair_kernel(own_ref, mine_ref, near_ref, far_ref, pair_ref, sent_ref):
    even = lax.rem(lax.axis_index("gy"), 2) == 0
    own = own_ref[...]
    mine = mine_ref[0:16, :].astype(f32)
    at = slice(META, META + 8)
    shape = (8, own.shape[1])
    spot = (iota(shape, 0) == 0) & (iota(shape, 1) < 2)
    for slot, other_ref in ((0, near_ref), (1, far_ref)):
        other = other_ref[...].astype(f32)
        total = own + other
        pair_ref[slot] = total
        right = even if slot == 0 else jnp.logical_not(even)
        meta = jnp.where(right, mine[at], other[at])
        pair_ref[slot, at, :] = jnp.where(spot, meta, total[at])
        sent_ref[slot] = pair_ref[slot].astype(bf16)


def pair_sums(own, mine, near, far):
    shape = (2,) + own.shape
    return pl.pallas_call(
        pair_kernel,
        in_specs=[vmem()] * 4,
        out_specs=[vmem()] * 2,
        out_shape=[jax.ShapeDtypeStruct(shape, f32), jax.ShapeDtypeStruct(shape, bf16)],
        compiler_params=pltpu.CompilerParams(vmem_limit_bytes=VMEM_LIMIT),
        cost_estimate=pl.CostEstimate(flops=4 * own.size, bytes_accessed=0, transcendentals=0),
        name="pair_sums",
    )(own, mine, near, far)


def split(x):
    high = x.astype(bf16)
    low = (x - high.astype(f32)).astype(bf16)
    return high, low


def unpacked(pk):
    frames = pk.shape[0]
    rest = frames - LANES
    first = LANES - rest
    shape = (LANES, LANES)
    row, lane = iota(shape, 0), iota(shape, 1)
    gap = jnp.zeros((first, LANES), f32)
    top = pk[:LANES]
    g11 = jnp.where(lane >= row, top, top.T)
    g21 = jnp.concatenate([pk[LANES:], gap], 0)
    low = jnp.concatenate([pk[first:LANES], gap], 0)
    low = jnp.where((lane <= row) & (row < rest), low, 0.0)
    g22 = jnp.where(lane <= row, low, low.T)
    return g11, g21.T, g21, g22


def spread(x, row):
    return jnp.broadcast_to(x[row : row + 1, :], (8, LANES))


def inverse_factor(a):
    count = K // 8
    sub, lane = iota((8, LANES), 0), iota((8, LANES), 1)
    base = (lane // K) * K
    rows = [a[8 * v : 8 * v + 8] for v in range(count)]
    inv = [jnp.where(sub + 8 * v == lane - base, 1.0, 0.0) for v in range(count)]
    for k0 in range(0, K, PANEL):
        cols = {
            k: {
                v: jnp.take_along_axis(rows[v], base + k, axis=1)
                for v in range(k0 // 8, count)
            }
            for k in range(k0, k0 + PANEL)
        }
        for j in range(k0, k0 + PANEL):
            vj, sj = j // 8, j % 8
            r = lax.rsqrt(spread(cols[j][vj], sj))
            fac = {v: cols[j][v] * r for v in range(vj, count)}
            fac[vj] = jnp.where(sub > sj, fac[vj], 0.0)
            for k in range(j + 1, k0 + PANEL):
                m = spread(fac[k // 8], k % 8)
                for v in range(k // 8, count):
                    cols[k][v] = cols[k][v] - fac[v] * m
            e = spread(inv[vj], sj) * r
            for v in range(vj, count):
                inv[v] = inv[v] - fac[v] * e
            inv[vj] = jnp.where(sub == sj, e, inv[vj])
            if k0 + PANEL < K:
                e = spread(rows[vj], sj) * r
                for v in range(vj, count):
                    rows[v] = rows[v] - fac[v] * e
    return jnp.concatenate(inv, 0)


def blockwise(parts_of):
    return jnp.concatenate([parts_of(b) for b in range(4)], 0)


def subspaces(rows, cols, sums_ref, near_ref, far_ref, start_ref, high_ref, low_ref, z_ref, v_ref):
    row, col = lax.axis_index("gx"), lax.axis_index("gy")
    scale = 1.0 / float(BZ * BZ * BZ * 4)
    group = iota((K, LANES), 1) // K
    ranks, counts = [], []
    s_high, s_low = split(start_ref[...])
    s_both = jnp.concatenate([s_high, s_low], 0)
    for b in range(4):
        slot, turn_x = b % 2, b // 2
        other_ref = near_ref if turn_x == 0 else far_ref
        other = other_ref[slot]
        pk = (sums_ref[slot] + other.astype(f32)) * scale
        g11, g12, g21, g22 = unpacked(pk)
        for ref, part in ((high_ref, 0), (low_ref, 1)):
            ref[b, :LANES, :LANES] = split(g11)[part]
            ref[b, :LANES, LANES:] = split(g12)[part]
            ref[b, LANES:, :LANES] = split(g21)[part]
            ref[b, LANES:, LANES:] = split(g22)[part]
        right = lax.rem(col, 2) == slot
        down = lax.rem(row, 2) == turn_x
        tile = jnp.where(
            down,
            sums_ref[slot, META : META + 8, :],
            other_ref[slot, 0:16, :].astype(f32)[META : META + 8],
        )
        last_y = jnp.where(right, cols - 1, 0)
        last_x = jnp.where(down, rows - 1, 0)
        there = jnp.where(col == last_y, 0.0, 1.0) * jnp.where(row == last_x, 0.0, 1.0)
        wide = (K, v_ref.shape[1])
        ranks.append(jnp.broadcast_to(tile[:1, 0:1] * there, wide))
        counts.append(jnp.broadcast_to(tile[:1, 1:2], wide))
    for b in range(4):
        both = jnp.dot(s_both, high_ref[b], preferred_element_type=f32)
        z_ref[K * b : K * b + K, :] = (
            both[:K] + both[K:] + jnp.dot(s_high, low_ref[b], preferred_element_type=f32)
        )

    def turn(t, carry):
        z_high, z_low = split(z_ref[...])
        zz = jnp.concatenate([z_high, z_low], 0)
        s = lax.dot_general(zz, zz, (((1,), (1,)), ((), ())), preferred_element_type=f32)
        half = 4 * K
        s = (s[:half, :half] + s[half:, half:]) + (s[:half, half:] + s[half:, :half])
        a = jnp.where(group == 0, s[:K], 0.0)
        for b in range(1, 4):
            a = jnp.where(group == b, s[K * b : K * b + K], a)
        moved = []
        for b in range(4):
            high = z_high[K * b : K * b + K]
            low = z_low[K * b : K * b + K]
            both = jnp.dot(
                jnp.concatenate([high, low], 0), high_ref[b], preferred_element_type=f32
            )
            moved.append(
                both[:K] + both[K:] + jnp.dot(high, low_ref[b], preferred_element_type=f32)
            )
        y_high, y_low = split(jnp.concatenate(moved, 0))
        yy = jnp.concatenate([y_high, y_low], 0)
        inv = inverse_factor(a)
        wide = blockwise(lambda b: jnp.where(group == b, inv, 0.0))
        i_high, i_low = split(wide)
        left = jnp.concatenate(
            [jnp.concatenate([i_high, i_high], 1), jnp.concatenate([i_low, i_low], 1)], 0
        )
        nxt = jnp.dot(left, yy, preferred_element_type=f32)
        z_ref[...] = nxt[:half] + nxt[half:]
        v = jnp.dot(left, zz, preferred_element_type=f32)
        v = v[:half] + v[half:]
        turns = (t + 1).astype(f32)
        for b in range(4):
            part = slice(K * b, K * b + K)
            v_ref[part, :] = jnp.where(counts[b] == turns, v[part], v_ref[part, :])
        return carry

    lax.fori_loop(0, ITERS, turn, 0)
    k = iota((K, v_ref.shape[1]), 0).astype(f32)
    return blockwise(lambda b: jnp.where(k < ranks[b], v_ref[K * b : K * b + K, :], 0.0)).astype(bf16)


def tents(rows, cols, span):
    row, col = lax.axis_index("gx"), lax.axis_index("gy")

    def share(far, position, at, last):
        first_edge = jnp.where(at == 0, 1.0, 0.0)
        last_edge = jnp.where(at == last, 1.0, 0.0)
        edge = jnp.maximum(first_edge, last_edge)
        tent = jnp.where(far, float(span) - position, position + 1.0) / float(span + 1)
        tent = tent * (1.0 - edge) + edge
        return tent * jnp.where(far, 1.0 - first_edge, 1.0 - last_edge)

    def along_x(offset):
        far = iota((8, LANES), 1) // (2 * K) != lax.rem(row, 2)
        return share(far, offset, row, rows - 1)

    group = iota((span, LANES), 1) // K
    far = group % 2 != lax.rem(col, 2)
    along_y = share(far, iota((span, LANES), 0).astype(f32), col, cols - 1)
    return along_x, along_y


def filter_kernel(
    rows,
    cols,
    span,
    sums_ref,
    near_ref,
    far_ref,
    start_ref,
    c_hbm,
    out_hbm,
    high_ref,
    low_ref,
    z_ref,
    v_ref,
    c_ref,
    out_ref,
    in_sems,
    out_sems,
):
    m, frames = c_ref.shape
    chunks = [pl.ds(i * PROJ_CHUNK, PROJ_CHUNK) for i in range(m // PROJ_CHUNK)]
    loads = [
        pltpu.make_async_copy(c_hbm.at[part], c_ref.at[part], in_sems.at[i])
        for i, part in enumerate(chunks)
    ]
    stores = [
        pltpu.make_async_copy(out_ref.at[part], out_hbm.at[part], out_sems.at[i])
        for i, part in enumerate(chunks)
    ]
    for load in loads:
        load.start()
    q = subspaces(rows, cols, sums_ref, near_ref, far_ref, start_ref, high_ref, low_ref, z_ref, v_ref)
    q = q[:, :frames]
    along_x, along_y = tents(rows, cols, span)
    area = span * BZ
    for load in loads:
        load.wait()
    for at in range(0, m, area):
        c = c_ref[at : at + area, :]
        p = lax.dot_general(c, q, (((1,), (1,)), ((), ())), preferred_element_type=f32)
        weight = along_y * along_x(float(at // area))[:1]
        p = p.reshape(span, BZ, LANES) * weight[:, None, :]
        p = p.reshape(area, LANES).astype(bf16)
        clutter = jnp.dot(p, q, preferred_element_type=f32)
        out_ref[at : at + area, :] = (c.astype(f32) - clutter).astype(bf16)
        if (at + area) % PROJ_CHUNK == 0:
            stores[at // PROJ_CHUNK].start()
    for store in stores:
        store.wait()


def filtered(voxels, sums, near, far, start, rows, cols, span):
    m, frames = voxels.shape
    return pl.pallas_call(
        functools.partial(filter_kernel, rows, cols, span),
        in_specs=[vmem()] * 4 + [hbm()],
        out_specs=hbm(),
        out_shape=jax.ShapeDtypeStruct((m, frames), bf16),
        scratch_shapes=[
            pltpu.VMEM((4, 2 * LANES, 2 * LANES), bf16),
            pltpu.VMEM((4, 2 * LANES, 2 * LANES), bf16),
            pltpu.VMEM((4 * K, 2 * LANES), f32),
            pltpu.VMEM((4 * K, 2 * LANES), f32),
            pltpu.VMEM((m, frames), bf16),
            pltpu.VMEM((m, frames), bf16),
            pltpu.SemaphoreType.DMA((m // PROJ_CHUNK,)),
            pltpu.SemaphoreType.DMA((m // PROJ_CHUNK,)),
        ],
        compiler_params=pltpu.CompilerParams(vmem_limit_bytes=VMEM_LIMIT),
        cost_estimate=pl.CostEstimate(
            flops=8 * m * frames * K * 4, bytes_accessed=4 * m * frames, transcendentals=0
        ),
        name="filtered",
    )(sums, near, far, start, voxels)


def partner(x, axis):
    n = lax.axis_size(axis)
    return lax.ppermute(x, axis, [(i, i ^ 1) for i in range(n)])


def outer_partner(x, axis):
    n = lax.axis_size(axis)
    return lax.ppermute(x, axis, [(i, ((i - 1) ^ 1) + 1) for i in range(1, n - 1)])


def handed_on(x):
    n = lax.axis_size("gy")
    route = [(i, i + 2) for i in range(0, n - 2, 2)] + [(i, i - 2) for i in range(3, n, 2)]
    return lax.ppermute(x, "gy", route)


def body(echoes, start, ranks, counts):
    span, _, depth, frames = echoes.shape
    rows, cols = lax.axis_size("gx"), lax.axis_size("gy")
    voxels = echoes.reshape(span * span * depth, frames)
    own = own_gram(voxels)
    own, ranks, counts = lax.optimization_barrier((own, ranks, counts))
    row, lane = iota(own.shape, 0), iota(own.shape, 1)
    rank = jnp.where((row == META) & (lane == 0), ranks[0, 0, 0].astype(f32), own)
    mine = jnp.where((row == META) & (lane == 1), counts[0, 0, 0].astype(f32), rank).astype(bf16)
    near = partner(mine, "gy")
    far = handed_on(near)
    pair, sent = pair_sums(own, mine, near, far)
    near = partner(sent, "gx")
    far = outer_partner(sent, "gx")
    basis = jnp.pad(start.T, ((0, 0), (0, 2 * LANES - frames)))
    out = filtered(voxels, pair, near, far, basis, rows, cols, span)
    return out.reshape(echoes.shape)


def solution(mesh):
    placed = (P("gx", "gy", None, None), P(), P("gx", "gy", None), P("gx", "gy", None))
    return jax.shard_map(
        body, mesh=mesh, in_specs=placed, out_specs=P("gx", "gy", None, None), check_vma=False
    )
```

```python
import functools

import jax
import jax.numpy as jnp
from jax import lax
from jax.experimental import pallas as pl
from jax.experimental.pallas import tpu as pltpu
from jax.sharding import PartitionSpec as P

BZ = 16
K = 32
ITERS = 4
LANES = 128
META = 8
PROJ_CHUNK = 512
VMEM_LIMIT = 24 * 1024 * 1024
META_FLOPS = 1_000_000_000
PANEL = 16

f32 = jnp.float32
bf16 = jnp.bfloat16


def iota(shape, dim):
    return lax.broadcasted_iota(jnp.int32, shape, dim)


def meta_kernel(rank_ref, count_ref, meta_ref):
    shape = meta_ref.shape
    row, lane = iota(shape, 0), iota(shape, 1)
    rank, count = rank_ref[0, 0, 0].astype(f32), count_ref[0, 0, 0].astype(f32)
    meta = jnp.where(lane == 0, rank, jnp.where(lane == 1, count, 0.0))
    meta_ref[...] = jnp.where(row == 0, meta, 0.0)


def meta_tile(rank, count):
    return pl.pallas_call(
        meta_kernel,
        in_specs=[pl.BlockSpec(memory_space=pltpu.SMEM)] * 2,
        out_specs=vmem(),
        out_shape=jax.ShapeDtypeStruct((8, LANES), f32),
        compiler_params=pltpu.CompilerParams(vmem_limit_bytes=VMEM_LIMIT),
        cost_estimate=pl.CostEstimate(flops=META_FLOPS, bytes_accessed=0, transcendentals=0),
        name="meta_tile",
    )(rank, count)


def gram_kernel(meta_ref, c_ref, own_ref, sent_ref, acc_ref):
    frames = c_ref.shape[1]
    c = c_ref[...]
    acc_ref[...] = lax.dot_general(c, c, (((0,), (0,)), ((), ())), preferred_element_type=f32)
    rest = frames - LANES
    first = LANES - rest
    own_ref[...] = acc_ref[:, :LANES]
    shape = (rest, rest)
    low = iota(shape, 1) <= iota(shape, 0)
    own_ref[first:LANES, :rest] = jnp.where(
        low, acc_ref[LANES:, LANES:], acc_ref[first:LANES, :rest]
    )
    tile = own_ref[META : META + 8, :]
    spot = (iota(tile.shape, 0) == 0) & (iota(tile.shape, 1) < 2)
    own_ref[META : META + 8, :] = jnp.where(spot, meta_ref[...], tile)
    sent_ref[...] = own_ref[...].astype(bf16)


def vmem():
    return pl.BlockSpec(memory_space=pltpu.VMEM)


def hbm():
    return pl.BlockSpec(memory_space=pltpu.HBM)


def own_gram(voxels, meta):
    m, frames = voxels.shape
    return pl.pallas_call(
        gram_kernel,
        in_specs=[vmem()] * 2,
        out_specs=[vmem()] * 2,
        out_shape=[
            jax.ShapeDtypeStruct((frames, LANES), f32),
            jax.ShapeDtypeStruct((frames, LANES), bf16),
        ],
        scratch_shapes=[pltpu.VMEM((frames, frames), f32)],
        compiler_params=pltpu.CompilerParams(vmem_limit_bytes=VMEM_LIMIT),
        cost_estimate=pl.CostEstimate(
            flops=2 * m * frames * frames, bytes_accessed=2 * m * frames, transcendentals=0
        ),
        name="own_gram",
    )(meta, voxels)


def pair_kernel(own_ref, mine_ref, near_ref, far_ref, pair_ref, sent_ref):
    even = lax.rem(lax.axis_index("gy"), 2) == 0
    own = own_ref[...]
    mine = mine_ref[0:16, :].astype(f32)
    at = slice(META, META + 8)
    shape = (8, own.shape[1])
    spot = (iota(shape, 0) == 0) & (iota(shape, 1) < 2)
    for slot, other_ref in ((0, near_ref), (1, far_ref)):
        other = other_ref[...].astype(f32)
        total = own + other
        pair_ref[slot] = total
        right = even if slot == 0 else jnp.logical_not(even)
        meta = jnp.where(right, mine[at], other[at])
        pair_ref[slot, at, :] = jnp.where(spot, meta, total[at])
        sent_ref[slot] = pair_ref[slot].astype(bf16)


def pair_sums(own, mine, near, far):
    shape = (2,) + own.shape
    return pl.pallas_call(
        pair_kernel,
        in_specs=[vmem()] * 4,
        out_specs=[vmem()] * 2,
        out_shape=[jax.ShapeDtypeStruct(shape, f32), jax.ShapeDtypeStruct(shape, bf16)],
        compiler_params=pltpu.CompilerParams(vmem_limit_bytes=VMEM_LIMIT),
        cost_estimate=pl.CostEstimate(flops=4 * own.size, bytes_accessed=0, transcendentals=0),
        name="pair_sums",
    )(own, mine, near, far)


def split(x):
    high = x.astype(bf16)
    low = (x - high.astype(f32)).astype(bf16)
    return high, low


def unpacked(pk):
    frames = pk.shape[0]
    rest = frames - LANES
    first = LANES - rest
    shape = (LANES, LANES)
    row, lane = iota(shape, 0), iota(shape, 1)
    gap = jnp.zeros((first, LANES), f32)
    top = pk[:LANES]
    g11 = jnp.where(lane >= row, top, top.T)
    g21 = jnp.concatenate([pk[LANES:], gap], 0)
    low = jnp.concatenate([pk[first:LANES], gap], 0)
    low = jnp.where((lane <= row) & (row < rest), low, 0.0)
    g22 = jnp.where(lane <= row, low, low.T)
    return g11, g21.T, g21, g22


def spread(x, row):
    return jnp.broadcast_to(x[row : row + 1, :], (8, LANES))


def inverse_factor(a):
    count = K // 8
    sub, lane = iota((8, LANES), 0), iota((8, LANES), 1)
    base = (lane // K) * K
    rows = [a[8 * v : 8 * v + 8] for v in range(count)]
    inv = [jnp.where(sub + 8 * v == lane - base, 1.0, 0.0) for v in range(count)]
    for k0 in range(0, K, PANEL):
        cols = {
            k: {
                v: jnp.take_along_axis(rows[v], base + k, axis=1)
                for v in range(k0 // 8, count)
            }
            for k in range(k0, k0 + PANEL)
        }
        for j in range(k0, k0 + PANEL):
            vj, sj = j // 8, j % 8
            r = lax.rsqrt(spread(cols[j][vj], sj))
            fac = {v: cols[j][v] * r for v in range(vj, count)}
            fac[vj] = jnp.where(sub > sj, fac[vj], 0.0)
            for k in range(j + 1, k0 + PANEL):
                m = spread(fac[k // 8], k % 8)
                for v in range(k // 8, count):
                    cols[k][v] = cols[k][v] - fac[v] * m
            e = spread(inv[vj], sj) * r
            for v in range(vj, count):
                inv[v] = inv[v] - fac[v] * e
            inv[vj] = jnp.where(sub == sj, e, inv[vj])
            if k0 + PANEL < K:
                e = spread(rows[vj], sj) * r
                for v in range(vj, count):
                    rows[v] = rows[v] - fac[v] * e
    return jnp.concatenate(inv, 0)


def blockwise(parts_of):
    return jnp.concatenate([parts_of(b) for b in range(4)], 0)


def subspaces(rows, cols, sums_ref, near_ref, far_ref, start_ref, high_ref, low_ref, z_ref, v_ref):
    row, col = lax.axis_index("gx"), lax.axis_index("gy")
    scale = 1.0 / float(BZ * BZ * BZ * 4)
    group = iota((K, LANES), 1) // K
    ranks, counts = [], []
    s_high, s_low = split(start_ref[...])
    s_both = jnp.concatenate([s_high, s_low], 0)
    for b in range(4):
        slot, turn_x = b % 2, b // 2
        other_ref = near_ref if turn_x == 0 else far_ref
        other = other_ref[slot]
        pk = (sums_ref[slot] + other.astype(f32)) * scale
        g11, g12, g21, g22 = unpacked(pk)
        for ref, part in ((high_ref, 0), (low_ref, 1)):
            ref[b, :LANES, :LANES] = split(g11)[part]
            ref[b, :LANES, LANES:] = split(g12)[part]
            ref[b, LANES:, :LANES] = split(g21)[part]
            ref[b, LANES:, LANES:] = split(g22)[part]
        right = lax.rem(col, 2) == slot
        down = lax.rem(row, 2) == turn_x
        tile = jnp.where(
            down,
            sums_ref[slot, META : META + 8, :],
            other_ref[slot, 0:16, :].astype(f32)[META : META + 8],
        )
        last_y = jnp.where(right, cols - 1, 0)
        last_x = jnp.where(down, rows - 1, 0)
        there = jnp.where(col == last_y, 0.0, 1.0) * jnp.where(row == last_x, 0.0, 1.0)
        wide = (K, v_ref.shape[1])
        ranks.append(jnp.broadcast_to(tile[:1, 0:1] * there, wide))
        counts.append(jnp.broadcast_to(tile[:1, 1:2], wide))
    for b in range(4):
        both = jnp.dot(s_both, high_ref[b], preferred_element_type=f32)
        z_ref[K * b : K * b + K, :] = (
            both[:K] + both[K:] + jnp.dot(s_high, low_ref[b], preferred_element_type=f32)
        )

    def turn(t, carry):
        z_high, z_low = split(z_ref[...])
        zz = jnp.concatenate([z_high, z_low], 0)
        s = lax.dot_general(zz, zz, (((1,), (1,)), ((), ())), preferred_element_type=f32)
        half = 4 * K
        s = (s[:half, :half] + s[half:, half:]) + (s[:half, half:] + s[half:, :half])
        a = jnp.where(group == 0, s[:K], 0.0)
        for b in range(1, 4):
            a = jnp.where(group == b, s[K * b : K * b + K], a)
        moved = []
        for b in range(4):
            high = z_high[K * b : K * b + K]
            low = z_low[K * b : K * b + K]
            both = jnp.dot(
                jnp.concatenate([high, low], 0), high_ref[b], preferred_element_type=f32
            )
            moved.append(
                both[:K] + both[K:] + jnp.dot(high, low_ref[b], preferred_element_type=f32)
            )
        y_high, y_low = split(jnp.concatenate(moved, 0))
        yy = jnp.concatenate([y_high, y_low], 0)
        inv = inverse_factor(a)
        wide = blockwise(lambda b: jnp.where(group == b, inv, 0.0))
        i_high, i_low = split(wide)
        left = jnp.concatenate(
            [jnp.concatenate([i_high, i_high], 1), jnp.concatenate([i_low, i_low], 1)], 0
        )
        nxt = jnp.dot(left, yy, preferred_element_type=f32)
        z_ref[...] = nxt[:half] + nxt[half:]
        v = jnp.dot(left, zz, preferred_element_type=f32)
        v = v[:half] + v[half:]
        turns = (t + 1).astype(f32)
        for b in range(4):
            part = slice(K * b, K * b + K)
            v_ref[part, :] = jnp.where(counts[b] == turns, v[part], v_ref[part, :])
        return carry

    lax.fori_loop(0, ITERS, turn, 0)
    k = iota((K, v_ref.shape[1]), 0).astype(f32)
    return blockwise(lambda b: jnp.where(k < ranks[b], v_ref[K * b : K * b + K, :], 0.0)).astype(bf16)


def tents(rows, cols, span):
    row, col = lax.axis_index("gx"), lax.axis_index("gy")

    def share(far, position, at, last):
        first_edge = jnp.where(at == 0, 1.0, 0.0)
        last_edge = jnp.where(at == last, 1.0, 0.0)
        edge = jnp.maximum(first_edge, last_edge)
        tent = jnp.where(far, float(span) - position, position + 1.0) / float(span + 1)
        tent = tent * (1.0 - edge) + edge
        return tent * jnp.where(far, 1.0 - first_edge, 1.0 - last_edge)

    def along_x(offset):
        far = iota((8, LANES), 1) // (2 * K) != lax.rem(row, 2)
        return share(far, offset, row, rows - 1)

    group = iota((span, LANES), 1) // K
    far = group % 2 != lax.rem(col, 2)
    along_y = share(far, iota((span, LANES), 0).astype(f32), col, cols - 1)
    return along_x, along_y


def filter_kernel(
    rows,
    cols,
    span,
    sums_ref,
    near_ref,
    far_ref,
    start_ref,
    c_ref,
    out_hbm,
    high_ref,
    low_ref,
    z_ref,
    v_ref,
    out_ref,
    out_sems,
):
    m, frames = c_ref.shape
    chunks = [pl.ds(i * PROJ_CHUNK, PROJ_CHUNK) for i in range(m // PROJ_CHUNK)]
    stores = [
        pltpu.make_async_copy(out_ref.at[part], out_hbm.at[part], out_sems.at[i])
        for i, part in enumerate(chunks)
    ]
    q = subspaces(rows, cols, sums_ref, near_ref, far_ref, start_ref, high_ref, low_ref, z_ref, v_ref)
    q = q[:, :frames]
    along_x, along_y = tents(rows, cols, span)
    area = span * BZ
    for at in range(0, m, area):
        c = c_ref[at : at + area, :]
        p = lax.dot_general(c, q, (((1,), (1,)), ((), ())), preferred_element_type=f32)
        weight = along_y * along_x(float(at // area))[:1]
        p = p.reshape(span, BZ, LANES) * weight[:, None, :]
        p = p.reshape(area, LANES).astype(bf16)
        clutter = jnp.dot(p, q, preferred_element_type=f32)
        out_ref[at : at + area, :] = (c.astype(f32) - clutter).astype(bf16)
        if (at + area) % PROJ_CHUNK == 0:
            stores[at // PROJ_CHUNK].start()
    for store in stores:
        store.wait()


def filtered(voxels, sums, near, far, start, rows, cols, span):
    m, frames = voxels.shape
    return pl.pallas_call(
        functools.partial(filter_kernel, rows, cols, span),
        in_specs=[vmem()] * 5,
        out_specs=hbm(),
        out_shape=jax.ShapeDtypeStruct((m, frames), bf16),
        scratch_shapes=[
            pltpu.VMEM((4, 2 * LANES, 2 * LANES), bf16),
            pltpu.VMEM((4, 2 * LANES, 2 * LANES), bf16),
            pltpu.VMEM((4 * K, 2 * LANES), f32),
            pltpu.VMEM((4 * K, 2 * LANES), f32),
            pltpu.VMEM((m, frames), bf16),
            pltpu.SemaphoreType.DMA((m // PROJ_CHUNK,)),
        ],
        compiler_params=pltpu.CompilerParams(vmem_limit_bytes=VMEM_LIMIT),
        cost_estimate=pl.CostEstimate(
            flops=8 * m * frames * K * 4, bytes_accessed=4 * m * frames, transcendentals=0
        ),
        name="filtered",
    )(sums, near, far, start, voxels)


def partner(x, axis):
    n = lax.axis_size(axis)
    return lax.ppermute(x, axis, [(i, i ^ 1) for i in range(n)])


def outer_partner(x, axis):
    n = lax.axis_size(axis)
    return lax.ppermute(x, axis, [(i, ((i - 1) ^ 1) + 1) for i in range(1, n - 1)])


def handed_on(x):
    n = lax.axis_size("gy")
    route = [(i, i + 2) for i in range(0, n - 2, 2)] + [(i, i - 2) for i in range(3, n, 2)]
    return lax.ppermute(x, "gy", route)


def body(echoes, start, ranks, counts):
    span, _, depth, frames = echoes.shape
    rows, cols = lax.axis_size("gx"), lax.axis_size("gy")
    voxels = echoes.reshape(span * span * depth, frames)
    own, mine = own_gram(voxels, meta_tile(ranks, counts))
    near = partner(mine, "gy")
    far = handed_on(near)
    pair, sent = pair_sums(own, mine, near, far)
    near = partner(sent, "gx")
    far = outer_partner(sent, "gx")
    basis = jnp.pad(start.T, ((0, 0), (0, 2 * LANES - frames)))
    out = filtered(voxels, pair, near, far, basis, rows, cols, span)
    return out.reshape(echoes.shape)


def solution(mesh):
    placed = (P("gx", "gy", None, None), P(), P("gx", "gy", None), P("gx", "gy", None))
    return jax.shard_map(
        body, mesh=mesh, in_specs=placed, out_specs=P("gx", "gy", None, None), check_vma=False
    )
```

```python
import functools

import jax
import jax.numpy as jnp
from jax import lax
from jax.experimental import pallas as pl
from jax.experimental.pallas import tpu as pltpu
from jax.sharding import PartitionSpec as P

BZ = 16
K = 32
ITERS = 4
LANES = 128
META = 8
PROJ_CHUNK = 512
VMEM_LIMIT = 24 * 1024 * 1024
META_FLOPS = 1_000_000_000
PANELS = (0, 20, K)

f32 = jnp.float32
bf16 = jnp.bfloat16


def iota(shape, dim):
    return lax.broadcasted_iota(jnp.int32, shape, dim)


def meta_kernel(rank_ref, count_ref, meta_ref):
    shape = meta_ref.shape
    row, lane = iota(shape, 0), iota(shape, 1)
    rank, count = rank_ref[0, 0, 0].astype(f32), count_ref[0, 0, 0].astype(f32)
    meta = jnp.where(lane == 0, rank, jnp.where(lane == 1, count, 0.0))
    meta_ref[...] = jnp.where(row == 0, meta, 0.0)


def meta_tile(rank, count):
    return pl.pallas_call(
        meta_kernel,
        in_specs=[pl.BlockSpec(memory_space=pltpu.SMEM)] * 2,
        out_specs=vmem(),
        out_shape=jax.ShapeDtypeStruct((8, LANES), f32),
        compiler_params=pltpu.CompilerParams(vmem_limit_bytes=VMEM_LIMIT),
        cost_estimate=pl.CostEstimate(flops=META_FLOPS, bytes_accessed=0, transcendentals=0),
        name="meta_tile",
    )(rank, count)


def gram_kernel(meta_ref, c_ref, own_ref, sent_ref, acc_ref):
    frames = c_ref.shape[1]
    c = c_ref[...]
    acc_ref[...] = lax.dot_general(c, c, (((0,), (0,)), ((), ())), preferred_element_type=f32)
    rest = frames - LANES
    first = LANES - rest
    own_ref[...] = acc_ref[:, :LANES]
    shape = (rest, rest)
    low = iota(shape, 1) <= iota(shape, 0)
    own_ref[first:LANES, :rest] = jnp.where(
        low, acc_ref[LANES:, LANES:], acc_ref[first:LANES, :rest]
    )
    tile = own_ref[META : META + 8, :]
    spot = (iota(tile.shape, 0) == 0) & (iota(tile.shape, 1) < 2)
    own_ref[META : META + 8, :] = jnp.where(spot, meta_ref[...], tile)
    sent_ref[...] = own_ref[...].astype(bf16)


def vmem():
    return pl.BlockSpec(memory_space=pltpu.VMEM)


def hbm():
    return pl.BlockSpec(memory_space=pltpu.HBM)


def own_gram(voxels, meta):
    m, frames = voxels.shape
    return pl.pallas_call(
        gram_kernel,
        in_specs=[vmem()] * 2,
        out_specs=[vmem()] * 2,
        out_shape=[
            jax.ShapeDtypeStruct((frames, LANES), f32),
            jax.ShapeDtypeStruct((frames, LANES), bf16),
        ],
        scratch_shapes=[pltpu.VMEM((frames, frames), f32)],
        compiler_params=pltpu.CompilerParams(vmem_limit_bytes=VMEM_LIMIT),
        cost_estimate=pl.CostEstimate(
            flops=2 * m * frames * frames, bytes_accessed=2 * m * frames, transcendentals=0
        ),
        name="own_gram",
    )(meta, voxels)


def pair_kernel(own_ref, mine_ref, near_ref, far_ref, pair_ref, sent_ref):
    even = lax.rem(lax.axis_index("gy"), 2) == 0
    own = own_ref[...]
    mine = mine_ref[0:16, :].astype(f32)
    at = slice(META, META + 8)
    shape = (8, own.shape[1])
    spot = (iota(shape, 0) == 0) & (iota(shape, 1) < 2)
    for slot, other_ref in ((0, near_ref), (1, far_ref)):
        other = other_ref[...].astype(f32)
        total = own + other
        pair_ref[slot] = total
        right = even if slot == 0 else jnp.logical_not(even)
        meta = jnp.where(right, mine[at], other[at])
        pair_ref[slot, at, :] = jnp.where(spot, meta, total[at])
        sent_ref[slot] = pair_ref[slot].astype(bf16)


def pair_sums(own, mine, near, far):
    shape = (2,) + own.shape
    return pl.pallas_call(
        pair_kernel,
        in_specs=[vmem()] * 4,
        out_specs=[vmem()] * 2,
        out_shape=[jax.ShapeDtypeStruct(shape, f32), jax.ShapeDtypeStruct(shape, bf16)],
        compiler_params=pltpu.CompilerParams(vmem_limit_bytes=VMEM_LIMIT),
        cost_estimate=pl.CostEstimate(flops=4 * own.size, bytes_accessed=0, transcendentals=0),
        name="pair_sums",
    )(own, mine, near, far)


def split(x):
    high = x.astype(bf16)
    low = (x - high.astype(f32)).astype(bf16)
    return high, low


def unpacked(pk):
    frames = pk.shape[0]
    rest = frames - LANES
    first = LANES - rest
    shape = (LANES, LANES)
    row, lane = iota(shape, 0), iota(shape, 1)
    gap = jnp.zeros((first, LANES), f32)
    top = pk[:LANES]
    g11 = jnp.where(lane >= row, top, top.T)
    g21 = jnp.concatenate([pk[LANES:], gap], 0)
    low = jnp.concatenate([pk[first:LANES], gap], 0)
    low = jnp.where((lane <= row) & (row < rest), low, 0.0)
    g22 = jnp.where(lane <= row, low, low.T)
    return g11, g21.T, g21, g22


def spread(x, row):
    return jnp.broadcast_to(x[row : row + 1, :], (8, LANES))


def inverse_factor(a):
    count = K // 8
    sub, lane = iota((8, LANES), 0), iota((8, LANES), 1)
    base = (lane // K) * K
    rows = [a[8 * v : 8 * v + 8] for v in range(count)]
    inv = [jnp.where(sub + 8 * v == lane - base, 1.0, 0.0) for v in range(count)]
    for k0, k1 in zip(PANELS, PANELS[1:]):
        cols = {
            k: {
                v: jnp.take_along_axis(rows[v], base + k, axis=1)
                for v in range(k0 // 8, count)
            }
            for k in range(k0, k1)
        }
        for j in range(k0, k1):
            vj, sj = j // 8, j % 8
            r = lax.rsqrt(spread(cols[j][vj], sj))
            fac = {v: cols[j][v] * r for v in range(vj, count)}
            fac[vj] = jnp.where(sub > sj, fac[vj], 0.0)
            for k in range(j + 1, k1):
                m = spread(fac[k // 8], k % 8)
                for v in range(k // 8, count):
                    cols[k][v] = cols[k][v] - fac[v] * m
            e = spread(inv[vj], sj) * r
            for v in range(vj, count):
                inv[v] = inv[v] - fac[v] * e
            inv[vj] = jnp.where(sub == sj, e, inv[vj])
            if k1 < K:
                e = spread(rows[vj], sj) * r
                for v in range(vj, count):
                    rows[v] = rows[v] - fac[v] * e
    return jnp.concatenate(inv, 0)


def blockwise(parts_of):
    return jnp.concatenate([parts_of(b) for b in range(4)], 0)


def subspaces(rows, cols, sums_ref, near_ref, far_ref, start_ref, high_ref, low_ref, v_ref):
    row, col = lax.axis_index("gx"), lax.axis_index("gy")
    scale = 1.0 / float(BZ * BZ * BZ * 4)
    group = iota((K, LANES), 1) // K
    ranks, counts = [], []
    s_high, s_low = split(start_ref[...])
    for b in range(4):
        slot, turn_x = b % 2, b // 2
        other_ref = near_ref if turn_x == 0 else far_ref
        other = other_ref[slot]
        pk = (sums_ref[slot] + other.astype(f32)) * scale
        g11, g12, g21, g22 = unpacked(pk)
        for ref, part in ((high_ref, 0), (low_ref, 1)):
            ref[b, :LANES, :LANES] = split(g11)[part]
            ref[b, :LANES, LANES:] = split(g12)[part]
            ref[b, LANES:, :LANES] = split(g21)[part]
            ref[b, LANES:, LANES:] = split(g22)[part]
        right = lax.rem(col, 2) == slot
        down = lax.rem(row, 2) == turn_x
        tile = jnp.where(
            down,
            sums_ref[slot, META : META + 8, :],
            other_ref[slot, 0:16, :].astype(f32)[META : META + 8],
        )
        last_y = jnp.where(right, cols - 1, 0)
        last_x = jnp.where(down, rows - 1, 0)
        there = jnp.where(col == last_y, 0.0, 1.0) * jnp.where(row == last_x, 0.0, 1.0)
        wide = (K, v_ref.shape[1])
        ranks.append(jnp.broadcast_to(tile[:1, 0:1] * there, wide))
        counts.append(jnp.broadcast_to(tile[:1, 1:2], wide))
    def moved(high, low, b):
        both = jnp.dot(jnp.concatenate([high, low], 0), high_ref[b], preferred_element_type=f32)
        return both[:K] + both[K:] + jnp.dot(high, low_ref[b], preferred_element_type=f32)

    half = 4 * K
    z = blockwise(lambda b: moved(s_high, s_low, b))
    for t in range(ITERS):
        z_high, z_low = split(z)
        zz = jnp.concatenate([z_high, z_low], 0)
        s = lax.dot_general(zz, zz, (((1,), (1,)), ((), ())), preferred_element_type=f32)
        s = (s[:half, :half] + s[half:, half:]) + (s[:half, half:] + s[half:, :half])
        a = jnp.where(group == 0, s[:K], 0.0)
        for b in range(1, 4):
            a = jnp.where(group == b, s[K * b : K * b + K], a)
        inv = inverse_factor(a)
        wide = blockwise(lambda b: jnp.where(group == b, inv, 0.0))
        i_high, i_low = split(wide)
        left = jnp.concatenate(
            [jnp.concatenate([i_high, i_high], 1), jnp.concatenate([i_low, i_low], 1)], 0
        )
        if t < ITERS - 1:
            parts = [slice(K * b, K * b + K) for b in range(4)]
            y = blockwise(lambda b: moved(z_high[parts[b]], z_low[parts[b]], b))
            nxt = jnp.dot(left, jnp.concatenate(split(y), 0), preferred_element_type=f32)
            z = nxt[:half] + nxt[half:]
        v = jnp.dot(left, zz, preferred_element_type=f32)
        v = v[:half] + v[half:]
        for b in range(4):
            part = slice(K * b, K * b + K)
            if t == 0:
                v_ref[part, :] = v[part]
            else:
                v_ref[part, :] = jnp.where(counts[b] > t, v[part], v_ref[part, :])
    k = iota((K, v_ref.shape[1]), 0).astype(f32)
    return blockwise(lambda b: jnp.where(k < ranks[b], v_ref[K * b : K * b + K, :], 0.0)).astype(bf16)


def tents(rows, cols, span):
    row, col = lax.axis_index("gx"), lax.axis_index("gy")

    def share(far, position, at, last):
        first_edge = jnp.where(at == 0, 1.0, 0.0)
        last_edge = jnp.where(at == last, 1.0, 0.0)
        edge = jnp.maximum(first_edge, last_edge)
        tent = jnp.where(far, float(span) - position, position + 1.0) / float(span + 1)
        tent = tent * (1.0 - edge) + edge
        return tent * jnp.where(far, 1.0 - first_edge, 1.0 - last_edge)

    def along_x(offset):
        far = iota((8, LANES), 1) // (2 * K) != lax.rem(row, 2)
        return share(far, offset, row, rows - 1)

    group = iota((span, LANES), 1) // K
    far = group % 2 != lax.rem(col, 2)
    along_y = share(far, iota((span, LANES), 0).astype(f32), col, cols - 1)
    return along_x, along_y


def filter_kernel(
    rows,
    cols,
    span,
    sums_ref,
    near_ref,
    far_ref,
    start_ref,
    c_ref,
    out_hbm,
    high_ref,
    low_ref,
    v_ref,
    out_ref,
    out_sems,
):
    m, frames = c_ref.shape
    chunks = [pl.ds(i * PROJ_CHUNK, PROJ_CHUNK) for i in range(m // PROJ_CHUNK)]
    stores = [
        pltpu.make_async_copy(out_ref.at[part], out_hbm.at[part], out_sems.at[i])
        for i, part in enumerate(chunks)
    ]
    q = subspaces(rows, cols, sums_ref, near_ref, far_ref, start_ref, high_ref, low_ref, v_ref)
    q = q[:, :frames]
    along_x, along_y = tents(rows, cols, span)
    area = span * BZ
    for at in range(0, m, area):
        c = c_ref[at : at + area, :]
        p = lax.dot_general(c, q, (((1,), (1,)), ((), ())), preferred_element_type=f32)
        weight = along_y * along_x(float(at // area))[:1]
        p = p.reshape(span, BZ, LANES) * weight[:, None, :]
        p = p.reshape(area, LANES).astype(bf16)
        clutter = jnp.dot(p, q, preferred_element_type=f32)
        out_ref[at : at + area, :] = (c.astype(f32) - clutter).astype(bf16)
        if (at + area) % PROJ_CHUNK == 0:
            stores[at // PROJ_CHUNK].start()
    for store in stores:
        store.wait()


def filtered(voxels, sums, near, far, start, rows, cols, span):
    m, frames = voxels.shape
    return pl.pallas_call(
        functools.partial(filter_kernel, rows, cols, span),
        in_specs=[vmem()] * 5,
        out_specs=hbm(),
        out_shape=jax.ShapeDtypeStruct((m, frames), bf16),
        scratch_shapes=[
            pltpu.VMEM((4, 2 * LANES, 2 * LANES), bf16),
            pltpu.VMEM((4, 2 * LANES, 2 * LANES), bf16),
            pltpu.VMEM((4 * K, 2 * LANES), f32),
            pltpu.VMEM((m, frames), bf16),
            pltpu.SemaphoreType.DMA((m // PROJ_CHUNK,)),
        ],
        compiler_params=pltpu.CompilerParams(vmem_limit_bytes=VMEM_LIMIT),
        cost_estimate=pl.CostEstimate(
            flops=8 * m * frames * K * 4, bytes_accessed=4 * m * frames, transcendentals=0
        ),
        name="filtered",
    )(sums, near, far, start, voxels)


def partner(x, axis):
    n = lax.axis_size(axis)
    return lax.ppermute(x, axis, [(i, i ^ 1) for i in range(n)])


def outer_partner(x, axis):
    n = lax.axis_size(axis)
    return lax.ppermute(x, axis, [(i, ((i - 1) ^ 1) + 1) for i in range(1, n - 1)])


def handed_on(x):
    n = lax.axis_size("gy")
    route = [(i, i + 2) for i in range(0, n - 2, 2)] + [(i, i - 2) for i in range(3, n, 2)]
    return lax.ppermute(x, "gy", route)


def body(echoes, start, ranks, counts):
    span, _, depth, frames = echoes.shape
    rows, cols = lax.axis_size("gx"), lax.axis_size("gy")
    voxels = echoes.reshape(span * span * depth, frames)
    own, mine = own_gram(voxels, meta_tile(ranks, counts))
    near = partner(mine, "gy")
    far = handed_on(near)
    pair, sent = pair_sums(own, mine, near, far)
    near = partner(sent, "gx")
    far = outer_partner(sent, "gx")
    basis = jnp.pad(start.T, ((0, 0), (0, 2 * LANES - frames)))
    out = filtered(voxels, pair, near, far, basis, rows, cols, span)
    return out.reshape(echoes.shape)


def solution(mesh):
    placed = (P("gx", "gy", None, None), P(), P("gx", "gy", None), P("gx", "gy", None))
    return jax.shard_map(
        body, mesh=mesh, in_specs=placed, out_specs=P("gx", "gy", None, None), check_vma=False
    )
```
